32 devices in a mesh: pb: 4 (over x, core), kv: 8 (over z, y).
Axes of the slice: x: 2, y: 2, z: 4, core: 2. Of those that a mesh axis runs over, the one named last changes fastest.
Arguments:
- queries: bfloat16 [32768, 256], P(('pb', 'kv')), may hold values from -64 to 64
- keys: bfloat16 [1024, 256], P('kv'), may hold values from -6 to 6
- values: bfloat16 [1024, 256], P('kv'), may hold values from -6 to 6
- dout: bfloat16 [32768, 256], P(('pb', 'kv')), may hold values from -256 to 256
Outputs:
- dq: float32 [32768, 256], P(('pb', 'kv'))
- dk: float32 [1024, 256], P('kv')
- dv: float32 [1024, 256], P('kv')
The draws below stay inside these ranges and needn't reach their ends.
All inputs are finite; a program needn't handle non-finite values.
Results may differ from the reference program's by a relative error of at most 0.0029.
Values may be sent and summed in bfloat16 or wider, within the bound.
No kernel may reach another device: no remote copies, remote signals or barrier semaphores. Data moves between devices by JAX's collectives and lax.ppermute only.
A program may use at most 64 MiB of HBM per device.

```python
import math
import jax
import jax.numpy as jnp
from jax import lax

H = 2
DH = 128
TQ = 32768
TK = 1024


def paired(key):
    key_draw = jax.random.fold_in(key, 101)
    query_draw = jax.random.fold_in(key, 202)
    keys_arr = jnp.clip(jax.random.normal(key_draw, (TK, H * DH), jnp.float32), -6.0, 6.0)
    queries_arr = jnp.clip(jax.random.normal(query_draw, (TQ, H * DH), jnp.float32), -6.0, 6.0)
    return (queries_arr, keys_arr)


def draw_queries(key, part):
    return paired(key)[0].astype(jnp.bfloat16)


def draw_keys(key, part):
    return paired(key)[1].astype(jnp.bfloat16)


def block_scale(key, shape, split, smallest, largest):
    level = 1.0
    for axis_at, shards_of in split:
        steps = jax.random.uniform(jax.random.fold_in(jax.random.fold_in(key, 6), axis_at), (shards_of,), jnp.float32, smallest / len(split), largest / len(split))
        level = level * jnp.repeat(jnp.exp(steps), shape[axis_at] // shards_of).reshape((-1,) + (1,) * (len(shape) - 1 - axis_at))
    return level


def gaussian(rng, dims, width, bound, split=(), dtype=jnp.bfloat16):
    array = width * jax.random.normal(rng, dims, jnp.float32)
    if split:
        array = array * block_scale(rng, dims, split, -0.22, 0.18)
    return jnp.clip(array, -bound, bound).astype(dtype)


def setup_inputs(seed: int = 0) -> dict:
    splits = jax.random.split(jax.random.key(seed), 5)
    queries = draw_queries(jax.random.fold_in(splits[4], 71), 0)
    keys = draw_keys(jax.random.fold_in(splits[4], 71), 0)
    values = gaussian(splits[2], (TK, H * DH), 1.0, 6.0, ((0, 8),))
    dout = gaussian(splits[3], (TQ, H * DH), 48.0, 256.0, ((0, 32),))
    return dict(queries=queries, keys=keys, values=values, dout=dout)


def reference(queries, keys, values, dout):
    score_scale = 1.0 / math.sqrt(DH)
    block_rows = math.gcd(TQ, 2048)
    blocks = TQ // block_rows
    key_heads = keys.astype(jnp.float32).reshape(TK, H, DH)
    value_heads = values.astype(jnp.float32).reshape(TK, H, DH)
    query_blocks = queries.astype(jnp.float32).reshape(blocks, block_rows, H, DH)
    grad_blocks = dout.astype(jnp.float32).reshape(blocks, block_rows, H, DH)

    def one_block(carry, pair):
        dk_total, dv_total = carry
        query_blk, grad_blk = pair
        logits = jnp.einsum('qhd,khd->hqk', query_blk, key_heads) * score_scale
        peak = lax.optimization_barrier(jnp.max(logits, axis=-1, keepdims=True))
        mass = lax.optimization_barrier(jnp.sum(jnp.exp(logits - peak), axis=-1, keepdims=True))
        lse = peak + jnp.log(mass)
        dprob = jnp.einsum('qhd,khd->hqk', grad_blk, value_heads)
        probs = jnp.exp(logits - lse)
        delta = lax.optimization_barrier(jnp.sum(probs * dprob, axis=-1, keepdims=True))
        dlogits = probs * (dprob - delta)
        probs_b = lax.optimization_barrier(probs.astype(jnp.bfloat16)).astype(jnp.float32)
        dlogits_b = lax.optimization_barrier(dlogits.astype(jnp.bfloat16)).astype(jnp.float32)
        dv_total = dv_total + jnp.einsum('hqk,qhd->khd', probs_b, grad_blk)
        dk_total = dk_total + jnp.einsum('hqk,qhd->khd', dlogits_b, query_blk) * score_scale
        dq_block = jnp.einsum('hqk,khd->qhd', dlogits_b, key_heads) * score_scale
        return ((dk_total, dv_total), dq_block)
    zeros = jnp.zeros((TK, H, DH), jnp.float32)
    (dk_total, dv_total), dq_blocks = lax.scan(one_block, (zeros, zeros), (query_blocks, grad_blocks))
    dq = dq_blocks.reshape(TQ, H * DH)
    return (dq, dk_total.reshape(TK, H * DH), dv_total.reshape(TK, H * DH))
```

```python
import math

import jax
import jax.numpy as jnp
from jax import lax
from jax.experimental import pallas as pl
from jax.experimental.pallas import tpu as pltpu
from jax.sharding import PartitionSpec as P

H = 2
DH = 128
W = H * DH


def swap(x, axis, bit):
    n = lax.axis_size(axis)
    return lax.ppermute(x, axis, [(i, i ^ bit) for i in range(n)])


def shift(x, axis, by):
    n = lax.axis_size(axis)
    return lax.ppermute(x, axis, [(i, (i + by) % n) for i in range(n)])


def attn_kernel(chunks, tile, q_ref, do_ref, *refs):
    kv = refs[:chunks]
    dq_ref = refs[chunks]
    outs = refs[chunks + 1 : 2 * chunks + 1]
    s_ref, dp_ref = refs[2 * chunks + 1 :]
    rows = kv[0].shape[0]
    scale = 1.0 / math.sqrt(DH)
    to_exp2 = scale * math.log2(math.e)
    step = pl.program_id(0)
    last = pl.num_programs(0) - 1
    nt = (((1,), (1,)), ((), ()))
    nn = (((1,), (0,)), ((), ()))
    tn = (((0,), (0,)), ((), ()))

    @pl.when(step == 0)
    def _():
        for o in outs:
            o[...] = jnp.zeros_like(o)

    for h in range(H):
        lo, hi = h * DH, (h + 1) * DH
        q = q_ref[:, lo:hi]
        do = do_ref[:, lo:hi]
        peak = None
        for c in range(chunks):
            s = lax.dot_general(kv[c][:, lo:hi], q, nt, preferred_element_type=jnp.float32) * to_exp2
            s_ref[c * rows : (c + 1) * rows, :] = s
            m = jnp.max(s, axis=0, keepdims=True)
            peak = m if peak is None else jnp.maximum(peak, m)
        mass = jnp.zeros((1, tile), jnp.float32)
        weighted = jnp.zeros((1, tile), jnp.float32)
        for c in range(chunks):
            dp = lax.dot_general(
                kv[c][:, W + lo : W + hi], do, nt, preferred_element_type=jnp.float32
            )
            p = jnp.exp2(s_ref[c * rows : (c + 1) * rows, :] - peak)
            s_ref[c * rows : (c + 1) * rows, :] = p
            dp_ref[c * rows : (c + 1) * rows, :] = dp
            mass = mass + jnp.sum(p, axis=0, keepdims=True)
            weighted = weighted + jnp.sum(p * dp, axis=0, keepdims=True)
        inv = 1.0 / mass
        delta = weighted * inv
        dq = jnp.zeros((tile, DH), jnp.float32)
        for c in range(chunks):
            p = s_ref[c * rows : (c + 1) * rows, :] * inv
            ds = (p * (dp_ref[c * rows : (c + 1) * rows, :] - delta)).astype(jnp.bfloat16)
            pb = p.astype(jnp.bfloat16)
            outs[c][:, W + lo : W + hi] += lax.dot_general(
                pb, do, nn, preferred_element_type=jnp.float32
            )
            outs[c][:, lo:hi] += lax.dot_general(ds, q, nn, preferred_element_type=jnp.float32)
            dq = dq + lax.dot_general(
                ds, kv[c][:, lo:hi], tn, preferred_element_type=jnp.float32
            )
        dq_ref[:, lo:hi] = dq * scale

    @pl.when(step == last)
    def _():
        for o in outs:
            o[:, :W] = o[:, :W] * scale


def attn(queries, dout, kv):
    rows_q = queries.shape[0]
    tile = math.gcd(rows_q, 256)
    chunks = len(kv)
    rows = kv[0].shape[0]
    flops = 10 * rows_q * rows * chunks * W
    by_tile = pl.BlockSpec((tile, W), lambda i: (i, 0))
    whole = pl.BlockSpec((rows, 2 * W), lambda i: (0, 0))
    return pl.pallas_call(
        lambda *refs: attn_kernel(chunks, tile, *refs),
        grid=(rows_q // tile,),
        in_specs=[by_tile, by_tile] + [whole] * chunks,
        out_specs=[by_tile] + [whole] * chunks,
        out_shape=[jax.ShapeDtypeStruct((rows_q, W), jnp.float32)]
        + [jax.ShapeDtypeStruct((rows, 2 * W), jnp.float32)] * chunks,
        scratch_shapes=[pltpu.VMEM((chunks * rows, tile), jnp.float32)] * 2,
        cost_estimate=pl.CostEstimate(
            flops=flops, bytes_accessed=8 * rows_q * W, transcendentals=0
        ),
    )(queries, dout, *kv)


def local(queries, keys, values, dout):
    n = lax.axis_size("kv")
    lines = n // 2
    core = lax.axis_index("pb") % 2
    half = keys.shape[0] // 2
    kv = jnp.concatenate([keys, values], axis=1)
    mine = lax.dynamic_slice_in_dim(kv, core * half, half, 0)
    near = jnp.concatenate([mine] + [shift(mine, "kv", 2 * j) for j in range(1, lines)], axis=0)
    far = swap(near, "kv", 1)
    near_o = swap(near, "pb", 1)
    far_o = swap(far, "pb", 1)

    dq, g_near, g_far, g_near_o, g_far_o = attn(queries, dout, (near, far, near_o, far_o))

    g_far = g_far + swap(g_far_o, "pb", 1)
    g_near = g_near + swap(g_near_o, "pb", 1)
    g_near = g_near + swap(g_far.astype(jnp.bfloat16), "kv", 1).astype(jnp.float32)
    total = g_near[:half]
    for j in range(1, lines):
        piece = g_near[j * half : (j + 1) * half].astype(jnp.bfloat16)
        total = total + shift(piece, "kv", -2 * j).astype(jnp.float32)
    for bit in range(1, lax.axis_size("pb").bit_length() - 1):
        total = total + swap(total, "pb", 1 << bit)
    other = swap(total, "pb", 1)
    first = jnp.where(core == 0, total, other)
    second = jnp.where(core == 0, other, total)
    both = jnp.concatenate([first, second], axis=0)
    return (dq, both[:, :W], both[:, W:])


def solution(mesh):
    return jax.shard_map(
        local,
        mesh=mesh,
        in_specs=(P(("pb", "kv"), None), P("kv", None), P("kv", None), P(("pb", "kv"), None)),
        out_specs=(P(("pb", "kv"), None), P("kv", None), P("kv", None)),
        check_vma=False,
    )
```

```python
import math

import jax
import jax.numpy as jnp
from jax import lax
from jax.experimental import pallas as pl
from jax.experimental.pallas import tpu as pltpu
from jax.sharding import PartitionSpec as P

H = 2
DH = 128
W = H * DH


def swap(x, axis, bit):
    n = lax.axis_size(axis)
    return lax.ppermute(x, axis, [(i, i ^ bit) for i in range(n)])


def shift(x, axis, by):
    n = lax.axis_size(axis)
    return lax.ppermute(x, axis, [(i, (i + by) % n) for i in range(n)])


def dot(a, b):
    return lax.dot_general(a, b, (((1,), (0,)), ((), ())), preferred_element_type=jnp.float32)


def attn_kernel(sizes, groups, tile, block, *refs):
    q_ref, do_ref, qt_ref, dot_ref = refs[:4]
    pieces = refs[4 : 4 + len(sizes)]
    dq_ref = refs[4 + len(sizes)]
    outs = refs[5 + len(sizes) : 5 + len(sizes) + len(groups)]
    kv_ref, kt_ref, p_ref, dp_ref = refs[5 + len(sizes) + len(groups) :]
    total = sum(sizes)
    scale = 1.0 / math.sqrt(DH)
    to_exp2 = scale * math.log2(math.e)
    step = pl.program_id(0)
    last = pl.num_programs(0) - 1
    spans = [slice(at, at + block) for at in range(0, total, block)]
    places = [(o, slice(at, at + block)) for o, g in zip(outs, groups) for at in range(0, g, block)]

    @pl.when(step == 0)
    def _():
        at = 0
        for piece, rows in zip(pieces, sizes):
            kv_ref[at : at + rows, :] = piece[...]
            at += rows
        for out in outs:
            out[...] = jnp.zeros_like(out)
        for span in spans:
            kt_ref[:, span] = kv_ref[span, :W].T

    for h in range(H):
        head = slice(h * DH, (h + 1) * DH)
        vhead = slice(W + h * DH, W + (h + 1) * DH)
        peak = None
        for span in spans:
            s = dot(kv_ref[span, head], qt_ref[head, :]) * to_exp2
            p_ref[span, :] = s
            m = jnp.max(s, axis=0, keepdims=True)
            peak = m if peak is None else jnp.maximum(peak, m)
        mass = jnp.zeros_like(peak)
        weighted = jnp.zeros_like(peak)
        for span in spans:
            dp = dot(kv_ref[span, vhead], dot_ref[head, :])
            p = jnp.exp2(p_ref[span, :] - peak)
            p_ref[span, :] = p
            dp_ref[span, :] = dp
            mass = mass + jnp.sum(p, axis=0, keepdims=True)
            weighted = weighted + jnp.sum(p * dp, axis=0, keepdims=True)
        inv = 1.0 / mass
        delta = weighted * inv
        dq = None
        for span, (out, part_rows) in zip(spans, places):
            p = p_ref[span, :] * inv
            ds = (p * (dp_ref[span, :] - delta)).astype(jnp.bfloat16)
            out[part_rows, vhead] += dot(p.astype(jnp.bfloat16), do_ref[:, head])
            out[part_rows, head] += dot(ds, q_ref[:, head])
            part = dot(kt_ref[head, span], ds)
            dq = part if dq is None else dq + part
        dq_ref[head, :] = dq * scale

    @pl.when(step == last)
    def _():
        for out in outs:
            out[:, :W] = out[:, :W] * scale


def attn(queries, dout, pieces, groups):
    rows_q = queries.shape[0]
    sizes = [p.shape[0] for p in pieces]
    total = sum(sizes)
    tile = math.gcd(rows_q, 1024 if total <= 1024 else 256)
    block = math.gcd(groups[0], 256)
    limit = 8 * total * tile + 6 * total * W + 20 * tile * W + 8 * 2**20
    row = pl.BlockSpec((tile, W), lambda i: (i, 0))
    col = pl.BlockSpec((W, tile), lambda i: (0, i))
    vmem = pl.BlockSpec(memory_space=pltpu.VMEM)
    return pl.pallas_call(
        lambda *refs: attn_kernel(sizes, groups, tile, block, *refs),
        grid=(rows_q // tile,),
        in_specs=[row, row, col, col]
        + [pl.BlockSpec(p.shape, lambda i: (0, 0)) for p in pieces],
        out_specs=[col] + [vmem] * len(groups),
        out_shape=[jax.ShapeDtypeStruct((W, rows_q), jnp.float32)]
        + [jax.ShapeDtypeStruct((g, 2 * W), jnp.float32) for g in groups],
        scratch_shapes=[
            pltpu.VMEM((total, 2 * W), jnp.bfloat16),
            pltpu.VMEM((W, total), jnp.bfloat16),
            pltpu.VMEM((total, tile), jnp.float32),
            pltpu.VMEM((total, tile), jnp.float32),
        ],
        compiler_params=pltpu.CompilerParams(vmem_limit_bytes=limit),
        cost_estimate=pl.CostEstimate(
            flops=10 * rows_q * total * W, bytes_accessed=8 * rows_q * W, transcendentals=0
        ),
    )(queries, dout, queries.T, dout.T, *pieces)


def hops(lines):
    return sorted(range(1, lines), key=lambda j: (-min(j, lines - j), j))


def local(queries, keys, values, dout):
    lines = lax.axis_size("kv") // 2
    core = lax.axis_index("pb") % 2
    half = keys.shape[0] // 2
    kv = jnp.concatenate([keys, values], axis=1)
    mine = lax.dynamic_slice_in_dim(kv, core * half, half, 0)
    order = hops(lines)
    near = [mine] + [shift(mine, "kv", 2 * j) for j in order]
    far = [swap(piece, "kv", 1) for piece in near]
    near_o = swap(jnp.concatenate(near, axis=0), "pb", 1)
    far_o = swap(jnp.concatenate(far, axis=0), "pb", 1)

    many = lines * half
    dq, g_far_o, g_near_o, g_far, g_near = attn(
        queries, dout, [far_o, near_o] + far + near, [many] * 4
    )
    g_far_o = swap(g_far_o, "pb", 1)
    g_near_o = swap(g_near_o, "pb", 1)

    def rows(x, k):
        return x[k * half : (k + 1) * half]

    def from_far(k):
        sent = (rows(g_far, k) + rows(g_far_o, k)).astype(jnp.bfloat16)
        return swap(sent, "kv", 1)

    arrived = {k: from_far(k) for k in list(range(1, lines)) + [0]}

    def merged(k):
        return rows(g_near, k) + rows(g_near_o, k) + arrived[k].astype(jnp.float32)

    parts = [shift(merged(k).astype(jnp.bfloat16), "kv", -2 * j) for k, j in enumerate(order, 1)]
    total = merged(0)
    for part in parts:
        total = total + part.astype(jnp.float32)
    for bit in range(1, lax.axis_size("pb").bit_length() - 1):
        total = total + swap(total, "pb", 1 << bit)
    other = swap(total, "pb", 1)
    first = jnp.where(core == 0, total, other)
    second = jnp.where(core == 0, other, total)
    both = jnp.concatenate([first, second], axis=0)
    return (dq.T, both[:, :W], both[:, W:])


def solution(mesh):
    return jax.shard_map(
        local,
        mesh=mesh,
        in_specs=(P(("pb", "kv"), None), P("kv", None), P("kv", None), P(("pb", "kv"), None)),
        out_specs=(P(("pb", "kv"), None), P("kv", None), P("kv", None)),
        check_vma=False,
    )
```

```python
import math

import jax
import jax.numpy as jnp
from jax import lax
from jax.experimental import pallas as pl
from jax.experimental.pallas import tpu as pltpu
from jax.sharding import PartitionSpec as P

H = 2
DH = 128
W = H * DH


def swap(x, axis, bit):
    n = lax.axis_size(axis)
    return lax.ppermute(x, axis, [(i, i ^ bit) for i in range(n)])


def shift(x, axis, by):
    n = lax.axis_size(axis)
    return lax.ppermute(x, axis, [(i, (i + by) % n) for i in range(n)])


def dot(a, b):
    return lax.dot_general(a, b, (((1,), (0,)), ((), ())), preferred_element_type=jnp.float32)


def attn_kernel(sizes, groups, tile, block, *refs):
    q_ref, do_ref, qt_ref, dot_ref = refs[:4]
    pieces = refs[4 : 4 + len(sizes)]
    dq_ref = refs[4 + len(sizes)]
    outs = refs[5 + len(sizes) : 5 + len(sizes) + len(groups)]
    kv_ref, kt_ref, p_ref, dp_ref = refs[5 + len(sizes) + len(groups) :]
    total = sum(sizes)
    scale = 1.0 / math.sqrt(DH)
    to_exp2 = scale * math.log2(math.e)
    step = pl.program_id(0)
    last = pl.num_programs(0) - 1
    spans = [slice(at, at + block) for at in range(0, total, block)]
    places = [(o, slice(at, at + block)) for o, g in zip(outs, groups) for at in range(0, g, block)]

    @pl.when(step == 0)
    def _():
        at = 0
        for piece, rows in zip(pieces, sizes):
            kv_ref[at : at + rows, :] = piece[...]
            at += rows
        for out in outs:
            out[...] = jnp.zeros_like(out)
        for span in spans:
            kt_ref[:, span] = kv_ref[span, :W].T

    for h in range(H):
        head = slice(h * DH, (h + 1) * DH)
        vhead = slice(W + h * DH, W + (h + 1) * DH)
        peak = None
        for span in spans:
            s = dot(kv_ref[span, head], qt_ref[head, :]) * to_exp2
            p_ref[span, :] = s
            m = jnp.max(s, axis=0, keepdims=True)
            peak = m if peak is None else jnp.maximum(peak, m)
        mass = jnp.zeros_like(peak)
        weighted = jnp.zeros_like(peak)
        for span in spans:
            dp = dot(kv_ref[span, vhead], dot_ref[head, :])
            p = jnp.exp2(p_ref[span, :] - peak)
            p_ref[span, :] = p
            dp_ref[span, :] = dp
            mass = mass + jnp.sum(p, axis=0, keepdims=True)
            weighted = weighted + jnp.sum(p * dp, axis=0, keepdims=True)
        inv = 1.0 / mass
        delta = weighted * inv
        dq = None
        for span, (out, part_rows) in zip(spans, places):
            p = p_ref[span, :] * inv
            ds = (p * (dp_ref[span, :] - delta)).astype(jnp.bfloat16)
            out[part_rows, vhead] += dot(p.astype(jnp.bfloat16), do_ref[:, head])
            out[part_rows, head] += dot(ds, q_ref[:, head])
            part = dot(kt_ref[head, span], ds)
            dq = part if dq is None else dq + part
        dq_ref[head, :] = dq * scale

    @pl.when(step == last)
    def _():
        for out in outs:
            out[:, :W] = out[:, :W] * scale


def attn(queries, dout, queries_t, dout_t, pieces, groups):
    rows_q = queries.shape[0]
    sizes = [p.shape[0] for p in pieces]
    total = sum(sizes)
    tile = math.gcd(rows_q, 1024 if total <= 1024 else 256)
    block = math.gcd(groups[0], 256)
    limit = 8 * total * tile + 6 * total * W + 20 * tile * W + 8 * 2**20
    row = pl.BlockSpec((tile, W), lambda i: (i, 0))
    col = pl.BlockSpec((W, tile), lambda i: (0, i))
    vmem = pl.BlockSpec(memory_space=pltpu.VMEM)
    return pl.pallas_call(
        lambda *refs: attn_kernel(sizes, groups, tile, block, *refs),
        grid=(rows_q // tile,),
        in_specs=[row, row, col, col]
        + [pl.BlockSpec(p.shape, lambda i: (0, 0)) for p in pieces],
        out_specs=[col] + [vmem] * len(groups),
        out_shape=[jax.ShapeDtypeStruct((W, rows_q), jnp.float32)]
        + [jax.ShapeDtypeStruct((g, 2 * W), jnp.float32) for g in groups],
        scratch_shapes=[
            pltpu.VMEM((total, 2 * W), jnp.bfloat16),
            pltpu.VMEM((W, total), jnp.bfloat16),
            pltpu.VMEM((total, tile), jnp.float32),
            pltpu.VMEM((total, tile), jnp.float32),
        ],
        compiler_params=pltpu.CompilerParams(vmem_limit_bytes=limit),
        cost_estimate=pl.CostEstimate(
            flops=10 * rows_q * total * W, bytes_accessed=8 * rows_q * W, transcendentals=0
        ),
    )(queries, dout, queries_t, dout_t, *pieces)


def hops(lines):
    return sorted(range(1, lines), key=lambda j: (-min(j, lines - j), j))


def local(queries, keys, values, dout):
    lines = lax.axis_size("kv") // 2
    core = lax.axis_index("pb") % 2
    half = keys.shape[0] // 2
    kv = jnp.concatenate([keys, values], axis=1)
    mine = lax.dynamic_slice_in_dim(kv, core * half, half, 0)
    order = hops(lines)
    near = [mine] + [shift(mine, "kv", 2 * j) for j in order]
    near[-1], queries_t, dout_t = lax.optimization_barrier((near[-1], queries.T, dout.T))
    far = [swap(piece, "kv", 1) for piece in near]
    near_o = swap(jnp.concatenate(near, axis=0), "pb", 1)
    far_o = swap(jnp.concatenate(far, axis=0), "pb", 1)

    many = lines * half
    dq, g_far_o, g_near_o, g_far, g_near = attn(
        queries, dout, queries_t, dout_t, [far_o, near_o] + far + near, [many] * 4
    )
    g_far_o = swap(g_far_o, "pb", 1)
    g_near_o = swap(g_near_o, "pb", 1)

    def rows(x, k):
        return x[k * half : (k + 1) * half]

    def from_far(k):
        sent = (rows(g_far, k) + rows(g_far_o, k)).astype(jnp.bfloat16)
        return swap(sent, "kv", 1)

    arrived = {k: from_far(k) for k in list(range(1, lines)) + [0]}

    def merged(k):
        return rows(g_near, k) + rows(g_near_o, k) + arrived[k].astype(jnp.float32)

    parts = []
    for k, j in enumerate(order, 1):
        sent = merged(k).astype(jnp.bfloat16)
        parts.append(shift(sent, "kv", -2 * j))
        after = (k + 1) % lines
        arrived[after], _ = lax.optimization_barrier((arrived[after], sent))
    total = merged(0)
    for part in parts:
        total = total + part.astype(jnp.float32)
    for bit in range(1, lax.axis_size("pb").bit_length() - 1):
        total = total + swap(total, "pb", 1 << bit)
    other = swap(total, "pb", 1)
    first = jnp.where(core == 0, total, other)
    second = jnp.where(core == 0, other, total)
    both = jnp.concatenate([first, second], axis=0)
    return (dq.T, both[:, :W], both[:, W:])


def solution(mesh):
    return jax.shard_map(
        local,
        mesh=mesh,
        in_specs=(P(("pb", "kv"), None), P("kv", None), P("kv", None), P(("pb", "kv"), None)),
        out_specs=(P(("pb", "kv"), None), P("kv", None), P("kv", None)),
        check_vma=False,
    )
```

```python
import math

import jax
import jax.numpy as jnp
from jax import lax
from jax.experimental import pallas as pl
from jax.experimental.pallas import tpu as pltpu
from jax.sharding import PartitionSpec as P


H = 2
DH = 128
W = H * DH


def swap(x, axis, bit):
    n = lax.axis_size(axis)
    return lax.ppermute(x, axis, [(i, i ^ bit) for i in range(n)])


def shift(x, axis, by):
    n = lax.axis_size(axis)
    return lax.ppermute(x, axis, [(i, (i + by) % n) for i in range(n)])


def dot(a, b):
    return lax.dot_general(a, b, (((1,), (0,)), ((), ())), preferred_element_type=jnp.float32)


def score_kernel(to_exp2, qt_ref, dot_ref, kv_ref, p_ref, dp_ref, stat_ref):
    rows = kv_ref.shape[0]
    for h in range(H):
        head = slice(h * DH, (h + 1) * DH)
        vhead = slice(W + h * DH, W + (h + 1) * DH)
        own = slice(h * rows, (h + 1) * rows)
        s = dot(kv_ref[:, head], qt_ref[head, :]) * to_exp2
        peak = jnp.max(s, axis=0, keepdims=True)
        p = jnp.exp2(s - peak)
        dp = dot(kv_ref[:, vhead], dot_ref[head, :])
        p_ref[own, :] = p
        dp_ref[own, :] = dp
        stat_ref[h : h + 1, :] = peak
        stat_ref[H + h : H + h + 1, :] = jnp.sum(p, axis=0, keepdims=True)
        stat_ref[2 * H + h : 2 * H + h + 1, :] = jnp.sum(p * dp, axis=0, keepdims=True)


def score(queries_t, dout_t, kv):
    rows, n = kv.shape[0], queries_t.shape[1]
    vmem = pl.BlockSpec(memory_space=pltpu.VMEM)
    big = jax.ShapeDtypeStruct((H * rows, n), jnp.float32)
    return pl.pallas_call(
        lambda *refs: score_kernel(math.log2(math.e) / math.sqrt(DH), *refs),
        in_specs=[vmem] * 3,
        out_specs=[vmem] * 3,
        out_shape=[big, big, jax.ShapeDtypeStruct((4 * H, n), jnp.float32)],
        compiler_params=pltpu.CompilerParams(vmem_limit_bytes=12 * 2**20),
        cost_estimate=pl.CostEstimate(
            flops=4 * n * rows * W, bytes_accessed=8 * n * W, transcendentals=0
        ),
    )(queries_t, dout_t, kv)


def attn_kernel(sizes, groups, early, block, *refs):
    q_ref, do_ref, qt_ref, dot_ref = refs[:4]
    pieces = refs[4 : 4 + len(sizes)]
    refs = refs[4 + len(sizes) :]
    scored = {at: refs[3 * e : 3 * e + 3] for e, at in enumerate(early)}
    refs = refs[3 * len(early) :]
    dq_ref = refs[0]
    outs = refs[1 : 1 + len(groups)]
    kv_ref, kt_ref, p_ref, dp_ref = refs[1 + len(groups) :]
    total = sum(sizes)
    scale = 1.0 / math.sqrt(DH)
    to_exp2 = scale * math.log2(math.e)
    step = pl.program_id(0)
    last = pl.num_programs(0) - 1
    spans = [slice(at, at + block) for at in range(0, total, block)]
    places = [
        (i, outs[i], slice(at, at + block))
        for i, g in enumerate(groups)
        for at in range(0, g, block)
    ]
    fresh = [span for span, place in zip(spans, places) if place[0] not in scored]

    @pl.when(step == 0)
    def _():
        at = 0
        for piece, rows in zip(pieces, sizes):
            kv_ref[at : at + rows, :] = piece[...]
            at += rows
        for out in outs:
            out[...] = jnp.zeros_like(out)
        for span in spans:
            kt_ref[:, span] = kv_ref[span, :W].T

    for h in range(H):
        head = slice(h * DH, (h + 1) * DH)
        vhead = slice(W + h * DH, W + (h + 1) * DH)
        peak = None
        for span in fresh:
            s = dot(kv_ref[span, head], qt_ref[head, :]) * to_exp2
            p_ref[span, :] = s
            m = jnp.max(s, axis=0, keepdims=True)
            peak = m if peak is None else jnp.maximum(peak, m)
        for _, _, stat in scored.values():
            peak = jnp.maximum(peak, stat[h : h + 1, :])
        mass = jnp.zeros_like(peak)
        weighted = jnp.zeros_like(peak)
        share = {}
        for i, (_, _, stat) in scored.items():
            share[i] = jnp.exp2(stat[h : h + 1, :] - peak)
            mass = mass + share[i] * stat[H + h : H + h + 1, :]
            weighted = weighted + share[i] * stat[2 * H + h : 2 * H + h + 1, :]
        for span in fresh:
            dp = dot(kv_ref[span, vhead], dot_ref[head, :])
            p = jnp.exp2(p_ref[span, :] - peak)
            p_ref[span, :] = p
            dp_ref[span, :] = dp
            mass = mass + jnp.sum(p, axis=0, keepdims=True)
            weighted = weighted + jnp.sum(p * dp, axis=0, keepdims=True)
        inv = 1.0 / mass
        delta = weighted * inv
        dq = None
        for span, (i, out, part_rows) in zip(spans, places):
            if i in scored:
                at = h * groups[i] + part_rows.start
                there = slice(at, at + block)
                p = scored[i][0][there, :] * (share[i] * inv)
                dp = scored[i][1][there, :]
            else:
                p = p_ref[span, :] * inv
                dp = dp_ref[span, :]
            ds = (p * (dp - delta)).astype(jnp.bfloat16)
            out[part_rows, vhead] += dot(p.astype(jnp.bfloat16), do_ref[:, head])
            out[part_rows, head] += dot(ds, q_ref[:, head])
            part = dot(kt_ref[head, span], ds)
            dq = part if dq is None else dq + part
        dq_ref[head, :] = dq * scale

    @pl.when(step == last)
    def _():
        for out in outs:
            out[:, :W] = out[:, :W] * scale


def attn(queries, dout, queries_t, dout_t, pieces, groups, scored):
    rows_q = queries.shape[0]
    sizes = [p.shape[0] for p in pieces]
    total = sum(sizes)
    tile = math.gcd(rows_q, 1024 if total <= 1024 else 256)
    block = math.gcd(groups[0], 256)
    limit = 8 * total * tile + 6 * total * W + 20 * tile * W + 8 * 2**20
    row = pl.BlockSpec((tile, W), lambda i: (i, 0))
    col = pl.BlockSpec((W, tile), lambda i: (0, i))
    vmem = pl.BlockSpec(memory_space=pltpu.VMEM)
    return pl.pallas_call(
        lambda *refs: attn_kernel(sizes, groups, list(scored), block, *refs),
        grid=(rows_q // tile,),
        in_specs=[row, row, col, col]
        + [pl.BlockSpec(p.shape, lambda i: (0, 0)) for p in pieces]
        + [vmem] * (3 * len(scored)),
        out_specs=[col] + [vmem] * len(groups),
        out_shape=[jax.ShapeDtypeStruct((W, rows_q), jnp.float32)]
        + [jax.ShapeDtypeStruct((g, 2 * W), jnp.float32) for g in groups],
        scratch_shapes=[
            pltpu.VMEM((total, 2 * W), jnp.bfloat16),
            pltpu.VMEM((W, total), jnp.bfloat16),
            pltpu.VMEM((total, tile), jnp.float32),
            pltpu.VMEM((total, tile), jnp.float32),
        ],
        compiler_params=pltpu.CompilerParams(vmem_limit_bytes=limit),
        cost_estimate=pl.CostEstimate(
            flops=10 * rows_q * total * W, bytes_accessed=8 * rows_q * W, transcendentals=0
        ),
    )(queries, dout, queries_t, dout_t, *pieces, *[x for triple in scored.values() for x in triple])


def hops(lines):
    return sorted(range(1, lines), key=lambda j: (-min(j, lines - j), j))


def program(queries, keys, values, dout):
    lines = lax.axis_size("kv") // 2
    core = lax.axis_index("pb") % 2
    half = keys.shape[0] // 2
    kv = jnp.concatenate([keys, values], axis=1)
    mine = lax.dynamic_slice_in_dim(kv, core * half, half, 0)
    order = hops(lines)
    near = [mine] + [shift(mine, "kv", 2 * j) for j in order]
    near[-1], queries_t, dout_t = lax.optimization_barrier((near[-1], queries.T, dout.T))
    far = []
    for piece in near:
        far.append(swap(piece, "kv", 1))
    near = jnp.concatenate(near, axis=0)
    near_o = swap(near, "pb", 1)
    many = lines * half
    scored = {}
    early = 4 * many <= queries.shape[0]
    if early:
        scored[3] = score(queries_t, dout_t, near)
        far[-1], _ = lax.optimization_barrier((far[-1], scored[3][2]))
    far_all = jnp.concatenate(far, axis=0)
    far_o = swap(far_all, "pb", 1)

    if early:
        late, _ = lax.optimization_barrier((near_o, far_all))
        scored[1] = score(queries_t, dout_t, late)
    dq, g_far_o, g_near_o, g_far, g_near = attn(
        queries, dout, queries_t, dout_t, [far_o, near_o, far_all, near], [many] * 4, scored
    )
    g_far_o = swap(g_far_o, "pb", 1)
    g_near_o = swap(g_near_o, "pb", 1)

    def rows(x, k):
        return x[k * half : (k + 1) * half]

    def from_far(k):
        sent = (rows(g_far, k) + rows(g_far_o, k)).astype(jnp.bfloat16)
        return swap(sent, "kv", 1)

    arrived = {k: from_far(k) for k in range(1, lines)}
    g_far, _ = lax.optimization_barrier((g_far, arrived[1]))
    arrived[0] = from_far(0)

    def merged(k):
        return rows(g_near, k) + rows(g_near_o, k) + arrived[k].astype(jnp.float32)

    parts = []
    for k, j in enumerate(order, 1):
        sent = merged(k).astype(jnp.bfloat16)
        parts.append(shift(sent, "kv", -2 * j))
        after = (k + 1) % lines
        arrived[after], _ = lax.optimization_barrier((arrived[after], sent))
    total = merged(0)
    for part in parts:
        total = total + part.astype(jnp.float32)
    for bit in range(1, lax.axis_size("pb").bit_length() - 1):
        total = total + swap(total, "pb", 1 << bit)
    other = swap(total, "pb", 1)
    first = jnp.where(core == 0, total, other)
    second = jnp.where(core == 0, other, total)
    both = jnp.concatenate([first, second], axis=0)
    return (dq.T, both[:, :W], both[:, W:])


def solution(mesh):
    return jax.shard_map(
        program,
        mesh=mesh,
        in_specs=(P(("pb", "kv"), None), P("kv", None), P("kv", None), P(("pb", "kv"), None)),
        out_specs=(P(("pb", "kv"), None), P("kv", None), P("kv", None)),
        check_vma=False,
    )
```

```python
import math

import jax
import jax.numpy as jnp
from jax import lax
from jax.experimental import pallas as pl
from jax.experimental.pallas import tpu as pltpu
from jax.sharding import PartitionSpec as P


H = 2
DH = 128
W = H * DH


def swap(x, axis, bit):
    n = lax.axis_size(axis)
    return lax.ppermute(x, axis, [(i, i ^ bit) for i in range(n)])


def shift(x, axis, by):
    n = lax.axis_size(axis)
    return lax.ppermute(x, axis, [(i, (i + by) % n) for i in range(n)])


def dot(a, b):
    return lax.dot_general(a, b, (((1,), (0,)), ((), ())), preferred_element_type=jnp.float32)


def score_kernel(to_exp2, qt_ref, dot_ref, kv_ref, p_ref, dp_ref, stat_ref):
    rows = kv_ref.shape[0]
    for h in range(H):
        head = slice(h * DH, (h + 1) * DH)
        vhead = slice(W + h * DH, W + (h + 1) * DH)
        own = slice(h * rows, (h + 1) * rows)
        s = dot(kv_ref[:, head], qt_ref[head, :]) * to_exp2
        peak = jnp.max(s, axis=0, keepdims=True)
        p = jnp.exp2(s - peak)
        dp = dot(kv_ref[:, vhead], dot_ref[head, :])
        p_ref[own, :] = p
        dp_ref[own, :] = dp
        stat_ref[h : h + 1, :] = peak
        stat_ref[H + h : H + h + 1, :] = jnp.sum(p, axis=0, keepdims=True)
        stat_ref[2 * H + h : 2 * H + h + 1, :] = jnp.sum(p * dp, axis=0, keepdims=True)


def score(queries_t, dout_t, kv):
    rows, n = kv.shape[0], queries_t.shape[1]
    vmem = pl.BlockSpec(memory_space=pltpu.VMEM)
    big = jax.ShapeDtypeStruct((H * rows, n), jnp.float32)
    return pl.pallas_call(
        lambda *refs: score_kernel(math.log2(math.e) / math.sqrt(DH), *refs),
        in_specs=[vmem] * 3,
        out_specs=[vmem] * 3,
        out_shape=[big, big, jax.ShapeDtypeStruct((4 * H, n), jnp.float32)],
        compiler_params=pltpu.CompilerParams(vmem_limit_bytes=12 * 2**20),
        cost_estimate=pl.CostEstimate(
            flops=4 * n * rows * W, bytes_accessed=8 * n * W, transcendentals=0
        ),
    )(queries_t, dout_t, kv)


def grad_kernel(*refs):
    q_ref, do_ref, kv_ref, p_ref, dp_ref, own_ref, stat_ref, old_ref, dq_ref, out_ref = refs
    rows = kv_ref.shape[0]
    scale = 1.0 / math.sqrt(DH)
    for h in range(H):
        head = slice(h * DH, (h + 1) * DH)
        vhead = slice(W + h * DH, W + (h + 1) * DH)
        there = slice(h * rows, (h + 1) * rows)
        inv = stat_ref[H + h : H + h + 1, :]
        delta = stat_ref[2 * H + h : 2 * H + h + 1, :]
        share = jnp.exp2(own_ref[h : h + 1, :] - stat_ref[h : h + 1, :])
        p = p_ref[there, :] * (share * inv)
        ds = (p * (dp_ref[there, :] - delta)).astype(jnp.bfloat16)
        out_ref[:, vhead] = dot(p.astype(jnp.bfloat16), do_ref[:, head])
        out_ref[:, head] = dot(ds, q_ref[:, head]) * scale
        dq_ref[head, :] = old_ref[head, :] + dot(kv_ref[:, head].T, ds) * scale


def grad(queries, dout, kv, p, dp, own, stat, dq):
    rows, n = kv.shape[0], queries.shape[0]
    vmem = pl.BlockSpec(memory_space=pltpu.VMEM)
    return pl.pallas_call(
        grad_kernel,
        in_specs=[vmem] * 8,
        out_specs=[vmem] * 2,
        out_shape=[
            jax.ShapeDtypeStruct((W, n), jnp.float32),
            jax.ShapeDtypeStruct((rows, 2 * W), jnp.float32),
        ],
        compiler_params=pltpu.CompilerParams(vmem_limit_bytes=12 * 2**20),
        cost_estimate=pl.CostEstimate(
            flops=6 * n * rows * W, bytes_accessed=8 * n * W, transcendentals=0
        ),
    )(queries, dout, kv, p, dp, own, stat, dq)


def attn_kernel(sizes, groups, early, held, block, *refs):
    q_ref, do_ref, qt_ref, dot_ref = refs[:4]
    pieces = refs[4 : 4 + len(sizes)]
    refs = refs[4 + len(sizes) :]
    scored = {at: refs[3 * e : 3 * e + 3] for e, at in enumerate(early)}
    refs = refs[3 * len(early) :]
    dq_ref = refs[0]
    shown = [i for i in range(len(groups)) if i not in held]
    outs = dict(zip(shown, refs[1:]))
    refs = refs[1 + len(shown) :]
    kept = {}
    for i in held:
        if i not in scored:
            kept[i], refs = refs[:2], refs[2:]
    if held:
        stat_ref, refs = refs[0], refs[1:]
    kv_ref, kt_ref, p_ref, dp_ref = refs
    total = sum(sizes)
    scale = 1.0 / math.sqrt(DH)
    to_exp2 = scale * math.log2(math.e)
    step = pl.program_id(0)
    last = pl.num_programs(0) - 1
    spans = [slice(at, at + block) for at in range(0, total, block)]
    places = [
        (i, slice(at, at + block))
        for i, g in enumerate(groups)
        for at in range(0, g, block)
    ]
    fresh = [(span, *place) for span, place in zip(spans, places) if place[0] not in scored]

    def room(h, span, i, part):
        if i in kept:
            at = h * groups[i] + part.start
            return (*kept[i], slice(at, at + block))
        return (p_ref, dp_ref, span)


    @pl.when(step == 0)
    def _():
        at = 0
        for piece, rows in zip(pieces, sizes):
            kv_ref[at : at + rows, :] = piece[...]
            at += rows
        for out in outs.values():
            out[...] = jnp.zeros_like(out)
        for span in spans:
            kt_ref[:, span] = kv_ref[span, :W].T

    for h in range(H):
        head = slice(h * DH, (h + 1) * DH)
        vhead = slice(W + h * DH, W + (h + 1) * DH)
        peak = None
        for span, i, part in fresh:
            p_at, dp_at, there = room(h, span, i, part)
            s = dot(kv_ref[span, head], qt_ref[head, :]) * to_exp2
            p_at[there, :] = s
            m = jnp.max(s, axis=0, keepdims=True)
            peak = m if peak is None else jnp.maximum(peak, m)
        for _, _, stat in scored.values():
            peak = jnp.maximum(peak, stat[h : h + 1, :])
        mass = jnp.zeros_like(peak)
        weighted = jnp.zeros_like(peak)
        share = {}
        for i, (_, _, stat) in scored.items():
            share[i] = jnp.exp2(stat[h : h + 1, :] - peak)
            mass = mass + share[i] * stat[H + h : H + h + 1, :]
            weighted = weighted + share[i] * stat[2 * H + h : 2 * H + h + 1, :]
        for span, i, part in fresh:
            p_at, dp_at, there = room(h, span, i, part)
            dp = dot(kv_ref[span, vhead], dot_ref[head, :])
            p = jnp.exp2(p_at[there, :] - peak)
            p_at[there, :] = p
            dp_at[there, :] = dp
            mass = mass + jnp.sum(p, axis=0, keepdims=True)
            weighted = weighted + jnp.sum(p * dp, axis=0, keepdims=True)
        inv = 1.0 / mass
        delta = weighted * inv
        if held:
            stat_ref[h : h + 1, :] = peak
            stat_ref[H + h : H + h + 1, :] = inv
            stat_ref[2 * H + h : 2 * H + h + 1, :] = delta
        dq = None
        for span, (i, part_rows) in zip(spans, places):
            if i in held:
                continue
            out = outs[i]
            if i in scored:
                at = h * groups[i] + part_rows.start
                there = slice(at, at + block)
                p = scored[i][0][there, :] * (share[i] * inv)
                dp = scored[i][1][there, :]
            else:
                p = p_ref[span, :] * inv
                dp = dp_ref[span, :]
            ds = (p * (dp - delta)).astype(jnp.bfloat16)
            out[part_rows, vhead] += dot(p.astype(jnp.bfloat16), do_ref[:, head])
            out[part_rows, head] += dot(ds, q_ref[:, head])
            more = dot(kt_ref[head, span], ds)
            dq = more if dq is None else dq + more
        dq_ref[head, :] = dq * scale

    @pl.when(step == last)
    def _():
        for out in outs.values():
            out[:, :W] = out[:, :W] * scale


def attn(queries, dout, queries_t, dout_t, pieces, groups, scored, held):
    rows_q = queries.shape[0]
    sizes = [p.shape[0] for p in pieces]
    total = sum(sizes)
    tile = math.gcd(rows_q, 1024 if total <= 1024 else 256)
    block = math.gcd(groups[0], 256)
    shapes = [(W, rows_q)] + [(g, 2 * W) for i, g in enumerate(groups) if i not in held]
    for i in held:
        if i not in scored:
            shapes += [(H * groups[i], rows_q)] * 2
    if held:
        shapes.append((4 * H, rows_q))
    limit = 8 * total * tile + 6 * total * W + 20 * tile * W + 8 * 2**20
    row = pl.BlockSpec((tile, W), lambda i: (i, 0))
    col = pl.BlockSpec((W, tile), lambda i: (0, i))
    vmem = pl.BlockSpec(memory_space=pltpu.VMEM)
    return pl.pallas_call(
        lambda *refs: attn_kernel(sizes, groups, list(scored), held, block, *refs),
        grid=(rows_q // tile,),
        in_specs=[row, row, col, col]
        + [pl.BlockSpec(p.shape, lambda i: (0, 0)) for p in pieces]
        + [vmem] * (3 * len(scored)),
        out_specs=[col] + [vmem] * (len(shapes) - 1),
        out_shape=[jax.ShapeDtypeStruct(shape, jnp.float32) for shape in shapes],
        scratch_shapes=[
            pltpu.VMEM((total, 2 * W), jnp.bfloat16),
            pltpu.VMEM((W, total), jnp.bfloat16),
            pltpu.VMEM((total, tile), jnp.float32),
            pltpu.VMEM((total, tile), jnp.float32),
        ],
        compiler_params=pltpu.CompilerParams(vmem_limit_bytes=limit),
        cost_estimate=pl.CostEstimate(
            flops=10 * rows_q * total * W, bytes_accessed=8 * rows_q * W, transcendentals=0
        ),
    )(queries, dout, queries_t, dout_t, *pieces, *[x for triple in scored.values() for x in triple])


def hops(lines):
    return sorted(range(1, lines), key=lambda j: (-min(j, lines - j), j))


def program(queries, keys, values, dout):
    lines = lax.axis_size("kv") // 2
    core = lax.axis_index("pb") % 2
    half = keys.shape[0] // 2
    kv = jnp.concatenate([keys, values], axis=1)
    mine = lax.dynamic_slice_in_dim(kv, core * half, half, 0)
    order = hops(lines)
    near = [mine] + [shift(mine, "kv", 2 * j) for j in order]
    near[-1], queries_t, dout_t = lax.optimization_barrier((near[-1], queries.T, dout.T))
    far = []
    for piece in near:
        far.append(swap(piece, "kv", 1))
    near = jnp.concatenate(near, axis=0)
    near_o = swap(near, "pb", 1)
    many = lines * half
    scored = {}
    early = 4 * many <= queries.shape[0]
    if early:
        scored[3] = score(queries_t, dout_t, near)
        far[-1], _ = lax.optimization_barrier((far[-1], scored[3][2]))
    far_all = jnp.concatenate(far, axis=0)
    far_o = swap(far_all, "pb", 1)

    if early:
        late, _ = lax.optimization_barrier((near_o, far_all))
        scored[1] = score(queries_t, dout_t, late)
    pieces, groups = [far_o, near_o, far_all, near], [many] * 4
    if early:
        dq, g_far_o, g_near_o, p, dp, stat = attn(
            queries, dout, queries_t, dout_t, pieces, groups, scored, [2, 3]
        )
        g_far_o = swap(g_far_o, "pb", 1)
        g_near_o = swap(g_near_o, "pb", 1)
        dq, g_far = grad(queries, dout, far_all, p, dp, stat, stat, dq)
        dq, g_near = grad(queries, dout, near, *scored[3], stat, dq)
    else:
        dq, g_far_o, g_near_o, g_far, g_near = attn(
            queries, dout, queries_t, dout_t, pieces, groups, scored, []
        )
        g_far_o = swap(g_far_o, "pb", 1)
        g_near_o = swap(g_near_o, "pb", 1)

    def rows(x, k):
        return x[k * half : (k + 1) * half]

    def from_far(k):
        sent = (rows(g_far, k) + rows(g_far_o, k)).astype(jnp.bfloat16)
        return swap(sent, "kv", 1)

    arrived = {}
    for k in list(range(1, lines)) + [0]:
        arrived[k] = from_far(k)

    def merged(k):
        return rows(g_near, k) + rows(g_near_o, k) + arrived[k].astype(jnp.float32)

    parts = []
    for k, j in enumerate(order, 1):
        sent = merged(k).astype(jnp.bfloat16)
        parts.append(shift(sent, "kv", -2 * j))
        after = (k + 1) % lines
        arrived[after], _ = lax.optimization_barrier((arrived[after], sent))
    total = merged(0)
    for part in parts:
        total = total + part.astype(jnp.float32)
    for bit in range(1, lax.axis_size("pb").bit_length() - 1):
        total = total + swap(total, "pb", 1 << bit)
    other = swap(total, "pb", 1)
    first = jnp.where(core == 0, total, other)
    second = jnp.where(core == 0, other, total)
    both = jnp.concatenate([first, second], axis=0)
    return (dq.T, both[:, :W], both[:, W:])


def solution(mesh):
    return jax.shard_map(
        program,
        mesh=mesh,
        in_specs=(P(("pb", "kv"), None), P("kv", None), P("kv", None), P(("pb", "kv"), None)),
        out_specs=(P(("pb", "kv"), None), P("kv", None), P("kv", None)),
        check_vma=False,
    )
```

```python
import math

import jax
import jax.numpy as jnp
from jax import lax
from jax.experimental import pallas as pl
from jax.experimental.pallas import tpu as pltpu
from jax.sharding import PartitionSpec as P


H = 2
DH = 128
W = H * DH


def swap(x, axis, bit):
    n = lax.axis_size(axis)
    return lax.ppermute(x, axis, [(i, i ^ bit) for i in range(n)])


def shift(x, axis, by):
    n = lax.axis_size(axis)
    return lax.ppermute(x, axis, [(i, (i + by) % n) for i in range(n)])


def dot(a, b):
    return lax.dot_general(a, b, (((1,), (0,)), ((), ())), preferred_element_type=jnp.float32)


def score_kernel(to_exp2, qt_ref, dot_ref, kv_ref, p_ref, dp_ref, stat_ref):
    rows = kv_ref.shape[0]
    for h in range(H):
        head = slice(h * DH, (h + 1) * DH)
        vhead = slice(W + h * DH, W + (h + 1) * DH)
        own = slice(h * rows, (h + 1) * rows)
        s = dot(kv_ref[:, head], qt_ref[head, :]) * to_exp2
        peak = jnp.max(s, axis=0, keepdims=True)
        p = jnp.exp2(s - peak)
        dp = dot(kv_ref[:, vhead], dot_ref[head, :])
        p_ref[own, :] = p
        dp_ref[own, :] = dp
        stat_ref[h : h + 1, :] = peak
        stat_ref[H + h : H + h + 1, :] = jnp.sum(p, axis=0, keepdims=True)
        stat_ref[2 * H + h : 2 * H + h + 1, :] = jnp.sum(p * dp, axis=0, keepdims=True)


def score(queries_t, dout_t, kv):
    rows, n = kv.shape[0], queries_t.shape[1]
    vmem = pl.BlockSpec(memory_space=pltpu.VMEM)
    big = jax.ShapeDtypeStruct((H * rows, n), jnp.float32)
    return pl.pallas_call(
        lambda *refs: score_kernel(math.log2(math.e) / math.sqrt(DH), *refs),
        in_specs=[vmem] * 3,
        out_specs=[vmem] * 3,
        out_shape=[big, big, jax.ShapeDtypeStruct((4 * H, n), jnp.float32)],
        compiler_params=pltpu.CompilerParams(vmem_limit_bytes=12 * 2**20),
        cost_estimate=pl.CostEstimate(
            flops=4 * n * rows * W, bytes_accessed=8 * n * W, transcendentals=0
        ),
    )(queries_t, dout_t, kv)


def grad_kernel(*refs):
    q_ref, do_ref, kv_ref, p_ref, dp_ref, own_ref, stat_ref, old_ref, dq_ref, out_ref = refs
    rows = kv_ref.shape[0]
    scale = 1.0 / math.sqrt(DH)
    for h in range(H):
        head = slice(h * DH, (h + 1) * DH)
        vhead = slice(W + h * DH, W + (h + 1) * DH)
        there = slice(h * rows, (h + 1) * rows)
        inv = stat_ref[H + h : H + h + 1, :]
        delta = stat_ref[2 * H + h : 2 * H + h + 1, :]
        share = jnp.exp2(own_ref[h : h + 1, :] - stat_ref[h : h + 1, :])
        p = p_ref[there, :] * (share * inv)
        ds = (p * (dp_ref[there, :] - delta)).astype(jnp.bfloat16)
        out_ref[:, vhead] = dot(p.astype(jnp.bfloat16), do_ref[:, head])
        out_ref[:, head] = dot(ds, q_ref[:, head]) * scale
        dq_ref[head, :] = old_ref[head, :] + dot(kv_ref[:, head].T, ds) * scale


def grad(queries, dout, kv, p, dp, own, stat, dq):
    rows, n = kv.shape[0], queries.shape[0]
    vmem = pl.BlockSpec(memory_space=pltpu.VMEM)
    return pl.pallas_call(
        grad_kernel,
        in_specs=[vmem] * 8,
        out_specs=[vmem] * 2,
        out_shape=[
            jax.ShapeDtypeStruct((W, n), jnp.float32),
            jax.ShapeDtypeStruct((rows, 2 * W), jnp.float32),
        ],
        compiler_params=pltpu.CompilerParams(vmem_limit_bytes=12 * 2**20),
        cost_estimate=pl.CostEstimate(
            flops=6 * n * rows * W, bytes_accessed=8 * n * W, transcendentals=0
        ),
    )(queries, dout, kv, p, dp, own, stat, dq)


def attn_kernel(sizes, groups, early, held, block, *refs):
    q_ref, do_ref, qt_ref, dot_ref = refs[:4]
    pieces = refs[4 : 4 + len(sizes)]
    refs = refs[4 + len(sizes) :]
    scored = {at: refs[3 * e : 3 * e + 3] for e, at in enumerate(early)}
    refs = refs[3 * len(early) :]
    dq_ref = refs[0]
    shown = [i for i in range(len(groups)) if i not in held]
    outs = dict(zip(shown, refs[1:]))
    refs = refs[1 + len(shown) :]
    kept = {}
    for i in held:
        if i not in scored:
            kept[i], refs = refs[:2], refs[2:]
    if held:
        stat_ref, refs = refs[0], refs[1:]
    kv_ref, kt_ref, p_ref, dp_ref = refs
    total = sum(sizes)
    scale = 1.0 / math.sqrt(DH)
    to_exp2 = scale * math.log2(math.e)
    step = pl.program_id(0)
    last = pl.num_programs(0) - 1
    spans = [slice(at, at + block) for at in range(0, total, block)]
    places = [
        (i, slice(at, at + block))
        for i, g in enumerate(groups)
        for at in range(0, g, block)
    ]
    fresh = [(span, *place) for span, place in zip(spans, places) if place[0] not in scored]

    def room(h, span, i, part):
        if i in kept:
            at = h * groups[i] + part.start
            return (*kept[i], slice(at, at + block))
        return (p_ref, dp_ref, span)


    @pl.when(step == 0)
    def _():
        at = 0
        for piece, rows in zip(pieces, sizes):
            kv_ref[at : at + rows, :] = piece[...]
            at += rows
        for out in outs.values():
            out[...] = jnp.zeros_like(out)
        for span in spans:
            kt_ref[:, span] = kv_ref[span, :W].T

    for h in range(H):
        head = slice(h * DH, (h + 1) * DH)
        vhead = slice(W + h * DH, W + (h + 1) * DH)
        peak = None
        for span, i, part in fresh:
            p_at, dp_at, there = room(h, span, i, part)
            s = dot(kv_ref[span, head], qt_ref[head, :]) * to_exp2
            p_at[there, :] = s
            m = jnp.max(s, axis=0, keepdims=True)
            peak = m if peak is None else jnp.maximum(peak, m)
        for _, _, stat in scored.values():
            peak = jnp.maximum(peak, stat[h : h + 1, :])
        mass = jnp.zeros_like(peak)
        weighted = jnp.zeros_like(peak)
        share = {}
        for i, (_, _, stat) in scored.items():
            share[i] = jnp.exp2(stat[h : h + 1, :] - peak)
            mass = mass + share[i] * stat[H + h : H + h + 1, :]
            weighted = weighted + share[i] * stat[2 * H + h : 2 * H + h + 1, :]
        for span, i, part in fresh:
            p_at, dp_at, there = room(h, span, i, part)
            dp = dot(kv_ref[span, vhead], dot_ref[head, :])
            p = jnp.exp2(p_at[there, :] - peak)
            p_at[there, :] = p
            dp_at[there, :] = dp
            mass = mass + jnp.sum(p, axis=0, keepdims=True)
            weighted = weighted + jnp.sum(p * dp, axis=0, keepdims=True)
        inv = 1.0 / mass
        delta = weighted * inv
        if held:
            stat_ref[h : h + 1, :] = peak
            stat_ref[H + h : H + h + 1, :] = inv
            stat_ref[2 * H + h : 2 * H + h + 1, :] = delta
        dq = None
        for span, (i, part_rows) in zip(spans, places):
            if i in held:
                continue
            out = outs[i]
            if i in scored:
                at = h * groups[i] + part_rows.start
                there = slice(at, at + block)
                p = scored[i][0][there, :] * (share[i] * inv)
                dp = scored[i][1][there, :]
            else:
                p = p_ref[span, :] * inv
                dp = dp_ref[span, :]
            ds = (p * (dp - delta)).astype(jnp.bfloat16)
            out[part_rows, vhead] += dot(p.astype(jnp.bfloat16), do_ref[:, head])
            out[part_rows, head] += dot(ds, q_ref[:, head])
            more = dot(kt_ref[head, span], ds)
            dq = more if dq is None else dq + more
        dq_ref[head, :] = dq * scale

    @pl.when(step == last)
    def _():
        for out in outs.values():
            out[:, :W] = out[:, :W] * scale


def attn(queries, dout, queries_t, dout_t, pieces, groups, scored, held):
    rows_q = queries.shape[0]
    sizes = [p.shape[0] for p in pieces]
    total = sum(sizes)
    tile = math.gcd(rows_q, 1024 if total <= 1024 else 256)
    block = math.gcd(groups[0], 256)
    shapes = [(W, rows_q)] + [(g, 2 * W) for i, g in enumerate(groups) if i not in held]
    for i in held:
        if i not in scored:
            shapes += [(H * groups[i], rows_q)] * 2
    if held:
        shapes.append((4 * H, rows_q))
    limit = 8 * total * tile + 6 * total * W + 20 * tile * W + 8 * 2**20
    row = pl.BlockSpec((tile, W), lambda i: (i, 0))
    col = pl.BlockSpec((W, tile), lambda i: (0, i))
    vmem = pl.BlockSpec(memory_space=pltpu.VMEM)
    return pl.pallas_call(
        lambda *refs: attn_kernel(sizes, groups, list(scored), held, block, *refs),
        grid=(rows_q // tile,),
        in_specs=[row, row, col, col]
        + [pl.BlockSpec(p.shape, lambda i: (0, 0)) for p in pieces]
        + [vmem] * (3 * len(scored)),
        out_specs=[col] + [vmem] * (len(shapes) - 1),
        out_shape=[jax.ShapeDtypeStruct(shape, jnp.float32) for shape in shapes],
        scratch_shapes=[
            pltpu.VMEM((total, 2 * W), jnp.bfloat16),
            pltpu.VMEM((W, total), jnp.bfloat16),
            pltpu.VMEM((total, tile), jnp.float32),
            pltpu.VMEM((total, tile), jnp.float32),
        ],
        compiler_params=pltpu.CompilerParams(vmem_limit_bytes=limit),
        cost_estimate=pl.CostEstimate(
            flops=10 * rows_q * total * W, bytes_accessed=8 * rows_q * W, transcendentals=0
        ),
    )(queries, dout, queries_t, dout_t, *pieces, *[x for triple in scored.values() for x in triple])


def hops(lines):
    return sorted(range(1, lines), key=lambda j: (-min(j, lines - j), j))


def program(queries, keys, values, dout):
    lines = lax.axis_size("kv") // 2
    core = lax.axis_index("pb") % 2
    half = keys.shape[0] // 2
    kv = jnp.concatenate([keys, values], axis=1)
    mine = lax.dynamic_slice_in_dim(kv, core * half, half, 0)
    order = hops(lines)
    near = [mine] + [shift(mine, "kv", 2 * j) for j in order]
    near[-1], queries_t, dout_t = lax.optimization_barrier((near[-1], queries.T, dout.T))
    far = []
    for piece in near:
        far.append(swap(piece, "kv", 1))
    near = jnp.concatenate(near, axis=0)
    near_o = swap(near, "pb", 1)
    many = lines * half
    scored = {}
    early = 4 * many <= queries.shape[0]
    if early:
        scored[3] = score(queries_t, dout_t, near)
        scored[1] = score(queries_t, dout_t, near_o)
        far, _ = lax.optimization_barrier((far, (scored[1][2], scored[3][2])))
    far_all = jnp.concatenate(far, axis=0)
    far_o = swap(far_all, "pb", 1)

    if early:
        scored[2] = score(queries_t, dout_t, far_all)
    pieces, groups = [far_o, near_o, far_all, near], [many] * 4
    if early:
        dq, g_far_o, g_near_o, stat = attn(
            queries, dout, queries_t, dout_t, pieces, groups, scored, [2, 3]
        )
        g_far_o = swap(g_far_o, "pb", 1)
        g_near_o = swap(g_near_o, "pb", 1)
        dq, g_far = grad(queries, dout, far_all, *scored[2], stat, dq)
        dq, g_near = grad(queries, dout, near, *scored[3], stat, dq)
    else:
        dq, g_far_o, g_near_o, g_far, g_near = attn(
            queries, dout, queries_t, dout_t, pieces, groups, scored, []
        )
        g_far_o = swap(g_far_o, "pb", 1)
        g_near_o = swap(g_near_o, "pb", 1)

    def rows(x, k):
        return x[k * half : (k + 1) * half]

    def from_far(k):
        sent = (rows(g_far, k) + rows(g_far_o, k)).astype(jnp.bfloat16)
        return swap(sent, "kv", 1)

    arrived = {}
    sends = list(range(lines - 1, 0, -1))
    for k in sends + [0]:
        arrived[k] = from_far(k)

    def merged(k):
        return rows(g_near, k) + rows(g_near_o, k) + arrived[k].astype(jnp.float32)

    parts = []
    for at, k in enumerate(sends):
        sent = merged(k).astype(jnp.bfloat16)
        parts.append(shift(sent, "kv", -2 * order[k - 1]))
        after = (sends + [0])[at + 1]
        arrived[after], _ = lax.optimization_barrier((arrived[after], sent))
    total = merged(0)
    for part in parts:
        total = total + part.astype(jnp.float32)
    for bit in range(1, lax.axis_size("pb").bit_length() - 1):
        total = total + swap(total, "pb", 1 << bit)
    other = swap(total, "pb", 1)
    first = jnp.where(core == 0, total, other)
    second = jnp.where(core == 0, other, total)
    both = jnp.concatenate([first, second], axis=0)
    return (dq.T, both[:, :W], both[:, W:])


def solution(mesh):
    return jax.shard_map(
        program,
        mesh=mesh,
        in_specs=(P(("pb", "kv"), None), P("kv", None), P("kv", None), P(("pb", "kv"), None)),
        out_specs=(P(("pb", "kv"), None), P("kv", None), P("kv", None)),
        check_vma=False,
    )
```

```python
import math

import jax
import jax.numpy as jnp
from jax import lax
from jax.experimental import pallas as pl
from jax.experimental.pallas import tpu as pltpu
from jax.sharding import PartitionSpec as P


H = 2
DH = 128
W = H * DH


def swap(x, axis, bit):
    n = lax.axis_size(axis)
    return lax.ppermute(x, axis, [(i, i ^ bit) for i in range(n)])


def shift(x, axis, by):
    n = lax.axis_size(axis)
    return lax.ppermute(x, axis, [(i, (i + by) % n) for i in range(n)])


def dot(a, b):
    return lax.dot_general(a, b, (((1,), (0,)), ((), ())), preferred_element_type=jnp.float32)


def score_kernel(to_exp2, qt_ref, dot_ref, kv_ref, p_ref, dp_ref, stat_ref):
    rows = kv_ref.shape[0]
    for h in range(H):
        head = slice(h * DH, (h + 1) * DH)
        vhead = slice(W + h * DH, W + (h + 1) * DH)
        own = slice(h * rows, (h + 1) * rows)
        s = dot(kv_ref[:, head], qt_ref[head, :]) * to_exp2
        peak = jnp.max(s, axis=0, keepdims=True)
        p = jnp.exp2(s - peak)
        dp = dot(kv_ref[:, vhead], dot_ref[head, :])
        p_ref[own, :] = p
        dp_ref[own, :] = dp
        stat_ref[h : h + 1, :] = peak
        stat_ref[H + h : H + h + 1, :] = jnp.sum(p, axis=0, keepdims=True)
        stat_ref[2 * H + h : 2 * H + h + 1, :] = jnp.sum(p * dp, axis=0, keepdims=True)


def score(queries_t, dout_t, kv):
    rows, n = kv.shape[0], queries_t.shape[1]
    vmem = pl.BlockSpec(memory_space=pltpu.VMEM)
    big = jax.ShapeDtypeStruct((H * rows, n), jnp.float32)
    return pl.pallas_call(
        lambda *refs: score_kernel(math.log2(math.e) / math.sqrt(DH), *refs),
        in_specs=[vmem] * 3,
        out_specs=[vmem] * 3,
        out_shape=[big, big, jax.ShapeDtypeStruct((4 * H, n), jnp.float32)],
        compiler_params=pltpu.CompilerParams(vmem_limit_bytes=12 * 2**20),
        cost_estimate=pl.CostEstimate(
            flops=4 * n * rows * W, bytes_accessed=8 * n * W, transcendentals=0
        ),
    )(queries_t, dout_t, kv)


def grad_kernel(*refs):
    q_ref, do_ref, kv_ref, p_ref, dp_ref, own_ref, stat_ref, old_ref, dq_ref, out_ref = refs
    rows = kv_ref.shape[0]
    scale = 1.0 / math.sqrt(DH)
    for h in range(H):
        head = slice(h * DH, (h + 1) * DH)
        vhead = slice(W + h * DH, W + (h + 1) * DH)
        there = slice(h * rows, (h + 1) * rows)
        inv = stat_ref[H + h : H + h + 1, :]
        delta = stat_ref[2 * H + h : 2 * H + h + 1, :]
        share = jnp.exp2(own_ref[h : h + 1, :] - stat_ref[h : h + 1, :])
        p = p_ref[there, :] * (share * inv)
        ds = (p * (dp_ref[there, :] - delta)).astype(jnp.bfloat16)
        out_ref[:, vhead] = dot(p.astype(jnp.bfloat16), do_ref[:, head])
        out_ref[:, head] = dot(ds, q_ref[:, head]) * scale
        dq_ref[head, :] = old_ref[head, :] + dot(kv_ref[:, head].T, ds) * scale


def grad(queries, dout, kv, p, dp, own, stat, dq):
    rows, n = kv.shape[0], queries.shape[0]
    vmem = pl.BlockSpec(memory_space=pltpu.VMEM)
    return pl.pallas_call(
        grad_kernel,
        in_specs=[vmem] * 8,
        out_specs=[vmem] * 2,
        out_shape=[
            jax.ShapeDtypeStruct((W, n), jnp.float32),
            jax.ShapeDtypeStruct((rows, 2 * W), jnp.float32),
        ],
        compiler_params=pltpu.CompilerParams(vmem_limit_bytes=12 * 2**20),
        cost_estimate=pl.CostEstimate(
            flops=6 * n * rows * W, bytes_accessed=8 * n * W, transcendentals=0
        ),
    )(queries, dout, kv, p, dp, own, stat, dq)


def attn_kernel(sizes, groups, early, held, block, *refs):
    q_ref, do_ref, qt_ref, dot_ref = refs[:4]
    pieces = refs[4 : 4 + len(sizes)]
    refs = refs[4 + len(sizes) :]
    scored = {at: refs[3 * e : 3 * e + 3] for e, at in enumerate(early)}
    refs = refs[3 * len(early) :]
    dq_ref = refs[0]
    shown = [i for i in range(len(groups)) if i not in held]
    outs = dict(zip(shown, refs[1:]))
    refs = refs[1 + len(shown) :]
    kept = {}
    for i in held:
        if i not in scored:
            kept[i], refs = refs[:2], refs[2:]
    if held:
        stat_ref, refs = refs[0], refs[1:]
    kv_ref, kt_ref, p_ref, dp_ref = refs
    total = sum(sizes)
    scale = 1.0 / math.sqrt(DH)
    to_exp2 = scale * math.log2(math.e)
    step = pl.program_id(0)
    last = pl.num_programs(0) - 1
    spans = [slice(at, at + block) for at in range(0, total, block)]
    places = [
        (i, slice(at, at + block))
        for i, g in enumerate(groups)
        for at in range(0, g, block)
    ]
    fresh = [(span, *place) for span, place in zip(spans, places) if place[0] not in scored]

    def room(h, span, i, part):
        if i in kept:
            at = h * groups[i] + part.start
            return (*kept[i], slice(at, at + block))
        return (p_ref, dp_ref, span)


    @pl.when(step == 0)
    def _():
        at = 0
        for piece, rows in zip(pieces, sizes):
            kv_ref[at : at + rows, :] = piece[...]
            at += rows
        for out in outs.values():
            out[...] = jnp.zeros_like(out)
        for span in spans:
            kt_ref[:, span] = kv_ref[span, :W].T

    for h in range(H):
        head = slice(h * DH, (h + 1) * DH)
        vhead = slice(W + h * DH, W + (h + 1) * DH)
        peak = None
        for span, i, part in fresh:
            p_at, dp_at, there = room(h, span, i, part)
            s = dot(kv_ref[span, head], qt_ref[head, :]) * to_exp2
            p_at[there, :] = s
            m = jnp.max(s, axis=0, keepdims=True)
            peak = m if peak is None else jnp.maximum(peak, m)
        for _, _, stat in scored.values():
            peak = jnp.maximum(peak, stat[h : h + 1, :])
        mass = jnp.zeros_like(peak)
        weighted = jnp.zeros_like(peak)
        share = {}
        for i, (_, _, stat) in scored.items():
            share[i] = jnp.exp2(stat[h : h + 1, :] - peak)
            mass = mass + share[i] * stat[H + h : H + h + 1, :]
            weighted = weighted + share[i] * stat[2 * H + h : 2 * H + h + 1, :]
        for span, i, part in fresh:
            p_at, dp_at, there = room(h, span, i, part)
            dp = dot(kv_ref[span, vhead], dot_ref[head, :])
            p = jnp.exp2(p_at[there, :] - peak)
            p_at[there, :] = p
            dp_at[there, :] = dp
            mass = mass + jnp.sum(p, axis=0, keepdims=True)
            weighted = weighted + jnp.sum(p * dp, axis=0, keepdims=True)
        inv = 1.0 / mass
        delta = weighted * inv
        if held:
            stat_ref[h : h + 1, :] = peak
            stat_ref[H + h : H + h + 1, :] = inv
            stat_ref[2 * H + h : 2 * H + h + 1, :] = delta
        dq = None
        for span, (i, part_rows) in zip(spans, places):
            if i in held:
                continue
            out = outs[i]
            if i in scored:
                at = h * groups[i] + part_rows.start
                there = slice(at, at + block)
                p = scored[i][0][there, :] * (share[i] * inv)
                dp = scored[i][1][there, :]
            else:
                p = p_ref[span, :] * inv
                dp = dp_ref[span, :]
            ds = (p * (dp - delta)).astype(jnp.bfloat16)
            out[part_rows, vhead] += dot(p.astype(jnp.bfloat16), do_ref[:, head])
            out[part_rows, head] += dot(ds, q_ref[:, head])
            more = dot(kt_ref[head, span], ds)
            dq = more if dq is None else dq + more
        dq_ref[head, :] = dq * scale

    @pl.when(step == last)
    def _():
        for out in outs.values():
            out[:, :W] = out[:, :W] * scale


def attn(queries, dout, queries_t, dout_t, pieces, groups, scored, held):
    rows_q = queries.shape[0]
    sizes = [p.shape[0] for p in pieces]
    total = sum(sizes)
    tile = math.gcd(rows_q, 1024 if total <= 1024 else 256)
    block = math.gcd(groups[0], 256)
    shapes = [(W, rows_q)] + [(g, 2 * W) for i, g in enumerate(groups) if i not in held]
    for i in held:
        if i not in scored:
            shapes += [(H * groups[i], rows_q)] * 2
    if held:
        shapes.append((4 * H, rows_q))
    limit = 8 * total * tile + 6 * total * W + 20 * tile * W + 8 * 2**20
    row = pl.BlockSpec((tile, W), lambda i: (i, 0))
    col = pl.BlockSpec((W, tile), lambda i: (0, i))
    vmem = pl.BlockSpec(memory_space=pltpu.VMEM)
    return pl.pallas_call(
        lambda *refs: attn_kernel(sizes, groups, list(scored), held, block, *refs),
        grid=(rows_q // tile,),
        in_specs=[row, row, col, col]
        + [pl.BlockSpec(p.shape, lambda i: (0, 0)) for p in pieces]
        + [vmem] * (3 * len(scored)),
        out_specs=[col] + [vmem] * (len(shapes) - 1),
        out_shape=[jax.ShapeDtypeStruct(shape, jnp.float32) for shape in shapes],
        scratch_shapes=[
            pltpu.VMEM((total, 2 * W), jnp.bfloat16),
            pltpu.VMEM((W, total), jnp.bfloat16),
            pltpu.VMEM((total, tile), jnp.float32),
            pltpu.VMEM((total, tile), jnp.float32),
        ],
        compiler_params=pltpu.CompilerParams(vmem_limit_bytes=limit),
        cost_estimate=pl.CostEstimate(
            flops=10 * rows_q * total * W, bytes_accessed=8 * rows_q * W, transcendentals=0
        ),
    )(queries, dout, queries_t, dout_t, *pieces, *[x for triple in scored.values() for x in triple])


def hops(lines):
    return sorted(range(1, lines), key=lambda j: (-min(j, lines - j), j))


def program(queries, keys, values, dout):
    lines = lax.axis_size("kv") // 2
    core = lax.axis_index("pb") % 2
    half = keys.shape[0] // 2
    kv = jnp.concatenate([keys, values], axis=1)
    mine = lax.dynamic_slice_in_dim(kv, core * half, half, 0)
    order = hops(lines)
    near = [mine] + [shift(mine, "kv", 2 * j) for j in order]
    near[-1], queries_t, dout_t = lax.optimization_barrier((near[-1], queries.T, dout.T))
    far = []
    for piece in near:
        far.append(swap(piece, "kv", 1))
    near = jnp.concatenate(near, axis=0)
    near_o = swap(near, "pb", 1)
    many = lines * half
    scored = {}
    early = 4 * many <= queries.shape[0]
    if early:
        scored[3] = score(queries_t, dout_t, near)
        scored[1] = score(queries_t, dout_t, near_o)
        far, _ = lax.optimization_barrier((far, (scored[1][2], scored[3][2])))
    far_all = jnp.concatenate(far, axis=0)
    far_o = swap(far_all, "pb", 1)

    if early:
        scored[2] = score(queries_t, dout_t, far_all)
    pieces, groups = [far_o, near_o, far_all, near], [many] * 4
    if early:
        dq, g_far_o, stat = attn(
            queries, dout, queries_t, dout_t, [far_o], [many], scored, [1, 2, 3]
        )
        g_far_o = swap(g_far_o, "pb", 1)
        dq, g_near_o = grad(queries, dout, near_o, *scored[1], stat, dq)
        g_near_o = swap(g_near_o, "pb", 1)
        dq, g_far = grad(queries, dout, far_all, *scored[2], stat, dq)
        dq, g_near = grad(queries, dout, near, *scored[3], stat, dq)
    else:
        dq, g_far_o, g_near_o, g_far, g_near = attn(
            queries, dout, queries_t, dout_t, pieces, groups, scored, []
        )
        g_far_o = swap(g_far_o, "pb", 1)
        g_near_o = swap(g_near_o, "pb", 1)

    def rows(x, k):
        return x[k * half : (k + 1) * half]

    def from_far(k):
        sent = (rows(g_far, k) + rows(g_far_o, k)).astype(jnp.bfloat16)
        return swap(sent, "kv", 1)

    arrived = {}
    sends = list(range(lines - 1, 0, -1))
    for k in sends + [0]:
        arrived[k] = from_far(k)

    def merged(k):
        return rows(g_near, k) + rows(g_near_o, k) + arrived[k].astype(jnp.float32)

    parts = []
    for at, k in enumerate(sends):
        sent = merged(k).astype(jnp.bfloat16)
        parts.append(shift(sent, "kv", -2 * order[k - 1]))
        after = (sends + [0])[at + 1]
        arrived[after], _ = lax.optimization_barrier((arrived[after], sent))
    total = merged(0)
    for part in parts:
        total = total + part.astype(jnp.float32)
    for bit in range(1, lax.axis_size("pb").bit_length() - 1):
        total = total + swap(total, "pb", 1 << bit)
    other = swap(total, "pb", 1)
    first = jnp.where(core == 0, total, other)
    second = jnp.where(core == 0, other, total)
    both = jnp.concatenate([first, second], axis=0)
    return (dq.T, both[:, :W], both[:, W:])


def solution(mesh):
    return jax.shard_map(
        program,
        mesh=mesh,
        in_specs=(P(("pb", "kv"), None), P("kv", None), P("kv", None), P(("pb", "kv"), None)),
        out_specs=(P(("pb", "kv"), None), P("kv", None), P("kv", None)),
        check_vma=False,
    )
```
